32 devices in a mesh: seq: 16 (over z, x, core), tp: 2 (over y).
Axes of the slice: x: 2, y: 2, z: 4, core: 2. Of those that a mesh axis runs over, the one named last changes fastest.
Arguments:
- tokens: bfloat16 [8192, 3584], P(('seq', 'tp')), may hold values from -6 to 6
- pre_gain: float32 [3584], replicated, may hold values from 0.25 to 1.75
- post_gain: float32 [3584], replicated, may hold values from 0.25 to 1.75
- w_query: bfloat16 [3584, 4096], P('seq', 'tp'), may hold values from -0.09375 to 0.09375
- key_matrix: bfloat16 [3584, 2048], P('seq', 'tp'), may hold values from -0.09375 to 0.09375
- value_matrix: bfloat16 [3584, 2048], P('seq', 'tp'), may hold values from -0.09375 to 0.09375
- w_out: bfloat16 [4096, 3584], P('tp', 'seq'), may hold values from -0.09375 to 0.09375
Outputs:
- block_out: bfloat16 [8192, 3584], P(('seq', 'tp'))
The draws below stay inside these ranges and needn't reach their ends.
All inputs are finite; a program needn't handle non-finite values.
Results may differ from the reference program's by a relative error of at most 0.014.
Values may be sent and summed in bfloat16 or wider, within the bound.
A program may use at most 128 MiB of HBM per device.

```python
import jax
import jax.numpy as jnp
from jax import lax

MODEL_WIDTH = 3584
QUERY_HEADS = 16
KEY_VALUE_HEADS = 8
HEAD_SIZE = 256
BLOCK_TOKENS = 512
TOKENS = 8192
N_SEQ = 16
N_TP = 2


def shard_levels(rng, shape, split, least, largest):
    def one(axis_at, blocks):
        steps = jax.random.uniform(jax.random.fold_in(jax.random.fold_in(rng, 6), axis_at), (blocks,), jnp.float32, least / len(split), largest / len(split))
        return jnp.repeat(jnp.exp(steps), shape[axis_at] // blocks).reshape((-1,) + (1,) * (len(shape) - axis_at - 1))

    factor_of = one(*split[0])
    for cut in split[1:]:
        factor_of = factor_of * one(*cut)
    return factor_of


def scatter_about(key, shape, deviation, limit, shards=(), held_as=jnp.bfloat16):
    result = jax.random.normal(key, shape, jnp.float32) * deviation
    if len(shards) > 0:
        result = shard_levels(key, shape, shards, -0.22, 0.18) * result
    return jnp.clip(result, min=-limit, max=limit).astype(held_as)


def setup_inputs(seed: int = 0) -> dict:
    splits = jax.random.split(jax.random.key(seed), 8)
    return {
        "tokens": scatter_about(splits[0], (TOKENS, MODEL_WIDTH), 1.0, 6.0, ((0, 32),)),
        "pre_gain": jnp.clip(1.0 + 0.15 * jax.random.normal(splits[1], (MODEL_WIDTH,), jnp.float32), 0.25, 1.75),
        "post_gain": jnp.clip(1.0 + 0.15 * jax.random.normal(splits[2], (MODEL_WIDTH,), jnp.float32), 0.25, 1.75),
        "w_query": scatter_about(splits[3], (MODEL_WIDTH, QUERY_HEADS * HEAD_SIZE), MODEL_WIDTH ** -0.5, 0.09375, ((0, 16), (1, 2))),
        "key_matrix": scatter_about(splits[4], (MODEL_WIDTH, KEY_VALUE_HEADS * HEAD_SIZE), MODEL_WIDTH ** -0.5, 0.09375, ((0, 16), (1, 2))),
        "value_matrix": scatter_about(splits[5], (MODEL_WIDTH, KEY_VALUE_HEADS * HEAD_SIZE), MODEL_WIDTH ** -0.5, 0.09375, ((0, 16), (1, 2))),
        "w_out": scatter_about(splits[6], (QUERY_HEADS * HEAD_SIZE, MODEL_WIDTH), (QUERY_HEADS * HEAD_SIZE) ** -0.5, 0.09375, ((0, 2), (1, 16))),
    }


def root_norm(values, gain):
    values = values.astype(jnp.float32)
    return values * lax.rsqrt(lax.optimization_barrier(jnp.mean(values * values, axis=-1, keepdims=True)) + 1e-06) * gain.astype(jnp.float32)

def rotate_halves(values, token_positions):
    row_count = values.shape[0]
    shaped = values.reshape(row_count, -1, HEAD_SIZE)
    half_dim = HEAD_SIZE // 2
    freq = 10000.0 ** (-(jnp.arange(half_dim).astype(jnp.float32) * 2.0 / HEAD_SIZE))
    angle = token_positions[:, None] * freq[None, :]
    cosine = jnp.cos(angle)[:, None, :]
    sine_part = jnp.sin(angle)[:, None, :]
    first = shaped[..., :half_dim]
    second = shaped[..., half_dim:]
    turned = jnp.concatenate([first * cosine - second * sine_part, second * cosine + first * sine_part], axis=-1)
    return turned.reshape(row_count, -1)

def reference(tokens, pre_gain, post_gain, w_query, key_matrix, value_matrix, w_out):
    repeat_heads = QUERY_HEADS // KEY_VALUE_HEADS
    normalized_input = root_norm(tokens, pre_gain).astype(jnp.bfloat16)
    token_positions = jnp.arange(TOKENS).astype(jnp.float32)
    key_window = jnp.dot(normalized_input, key_matrix, preferred_element_type=jnp.float32)
    key_window = rotate_halves(key_window, token_positions).astype(jnp.bfloat16).reshape(N_SEQ, BLOCK_TOKENS, KEY_VALUE_HEADS, HEAD_SIZE)
    value_window = jnp.dot(normalized_input, value_matrix, preferred_element_type=jnp.float32).astype(jnp.bfloat16).reshape(N_SEQ, BLOCK_TOKENS, KEY_VALUE_HEADS, HEAD_SIZE)
    blank_rows = jnp.zeros((1, BLOCK_TOKENS, KEY_VALUE_HEADS, HEAD_SIZE), jnp.bfloat16)
    keys_prior = jnp.concatenate([blank_rows, key_window[:-1]], axis=0)
    vals_prior = jnp.concatenate([blank_rows, value_window[:-1]], axis=0)
    normed_blocks = normalized_input.reshape(N_SEQ, BLOCK_TOKENS, MODEL_WIDTH)
    token_blocks = tokens.reshape(N_SEQ, BLOCK_TOKENS, MODEL_WIDTH)
    out_groups = w_out.astype(jnp.float32).reshape(N_TP, QUERY_HEADS * HEAD_SIZE // N_TP, MODEL_WIDTH)

    def one_block(block_index):
        rows = normed_blocks[block_index]
        offset_pos = block_index * BLOCK_TOKENS
        local_pos = (offset_pos + jnp.arange(BLOCK_TOKENS).astype(jnp.int32)).astype(jnp.float32)
        raw_q = jnp.dot(rows, w_query, preferred_element_type=jnp.float32)
        query_rows = (rotate_halves(raw_q, local_pos) * HEAD_SIZE ** (-0.5)).astype(jnp.bfloat16)
        query_rows = query_rows.reshape(BLOCK_TOKENS, KEY_VALUE_HEADS, repeat_heads, HEAD_SIZE).astype(jnp.float32)
        key_current = jnp.concatenate([keys_prior[block_index], key_window[block_index]], axis=0).astype(jnp.float32)
        value_current = jnp.concatenate([vals_prior[block_index], value_window[block_index]], axis=0).astype(jnp.float32)
        attention_scores = jnp.einsum('cwap,bwp->wacb', query_rows, key_current)
        query_idx = jnp.arange(BLOCK_TOKENS).astype(jnp.int32)[:, None]
        key_idx = jnp.arange(2 * BLOCK_TOKENS).astype(jnp.int32)[None, :]
        key_pos = offset_pos - BLOCK_TOKENS + key_idx
        allowed = (key_idx > query_idx) & (key_idx <= query_idx + BLOCK_TOKENS) & (key_pos >= 0)
        weights = jnp.where(allowed, jnp.exp(attention_scores), 0.0)
        denominator = lax.optimization_barrier(jnp.sum(weights, axis=-1))
        weight_narrow = weights.astype(jnp.bfloat16).astype(jnp.float32)
        reduced_output = jnp.einsum('bpqu,ubm->qbpm', weight_narrow, value_current)
        attended = (reduced_output / jnp.transpose(denominator, (2, 0, 1))[..., None]).astype(jnp.bfloat16)
        attended = attended.reshape(BLOCK_TOKENS, N_TP, QUERY_HEADS * HEAD_SIZE // N_TP).astype(jnp.float32)
        partial_value = jnp.einsum('tgc,gcd->gtd', attended, out_groups).astype(jnp.bfloat16)
        partial_value = lax.optimization_barrier(partial_value)
        projected = lax.optimization_barrier(jnp.sum(partial_value.astype(jnp.float32), axis=0))
        mixed = root_norm(projected, post_gain)
        return (token_blocks[block_index].astype(jnp.float32) + mixed).astype(jnp.bfloat16)
    outputs = lax.map(one_block, jnp.arange(N_SEQ).astype(jnp.int32))
    return outputs.reshape(TOKENS, MODEL_WIDTH)
```

```python
import jax
import jax.numpy as jnp
from jax import lax
from jax.sharding import PartitionSpec as P

HEAD_SIZE = 256
PLANE = 4


def from_behind(x, axis, by):
    length = lax.axis_size(axis)
    pairs = [(i, i + by) for i in range(length) if 0 <= i + by < length]
    return lax.ppermute(x, axis, pairs)


def swap_seq(x, bits):
    return lax.ppermute(x, "seq", [(i, i ^ bits) for i in range(lax.axis_size("seq"))])


def swap_tp(x):
    return lax.ppermute(x, "tp", [(0, 1), (1, 0)])


def root_norm(values, gain):
    values = values.astype(jnp.float32)
    return values * lax.rsqrt(jnp.mean(values * values, axis=-1, keepdims=True) + 1e-06) * gain


def rotate_halves(values, token_positions):
    row_count = values.shape[0]
    shaped = values.reshape(row_count, -1, HEAD_SIZE)
    half_dim = HEAD_SIZE // 2
    freq = 10000.0 ** (-(jnp.arange(half_dim).astype(jnp.float32) * 2.0 / HEAD_SIZE))
    angle = token_positions[:, None] * freq[None, :]
    cosine = jnp.cos(angle)[:, None, :]
    sine_part = jnp.sin(angle)[:, None, :]
    first = shaped[..., :half_dim]
    second = shaped[..., half_dim:]
    turned = jnp.concatenate(
        [first * cosine - second * sine_part, second * cosine + first * sine_part], axis=-1
    )
    return turned.reshape(row_count, -1)


def attend(query_rows, keys_now, vals_now, keys_prior, vals_prior, offset_pos):
    length = query_rows.shape[0]
    kv_heads = keys_now.shape[1] // HEAD_SIZE
    repeat_heads = query_rows.shape[1] // (HEAD_SIZE * kv_heads)
    query_grouped = query_rows.reshape(length, kv_heads, repeat_heads, HEAD_SIZE)
    key_current = jnp.concatenate([keys_prior, keys_now], axis=0).reshape(
        2 * length, kv_heads, HEAD_SIZE
    )
    value_current = jnp.concatenate([vals_prior, vals_now], axis=0).reshape(
        2 * length, kv_heads, HEAD_SIZE
    )
    attention_scores = jnp.einsum(
        "cwap,bwp->wacb", query_grouped, key_current, preferred_element_type=jnp.float32
    )
    query_idx = jnp.arange(length)[:, None]
    key_idx = jnp.arange(2 * length)[None, :]
    key_pos = offset_pos - length + key_idx
    allowed = (key_idx > query_idx) & (key_idx <= query_idx + length) & (key_pos >= 0)
    weights = jnp.where(allowed, jnp.exp(attention_scores), 0.0)
    denominator = jnp.sum(weights, axis=-1)
    weight_narrow = weights.astype(jnp.bfloat16)
    reduced_output = jnp.einsum(
        "bpqu,ubm->qbpm", weight_narrow, value_current, preferred_element_type=jnp.float32
    )
    attended = reduced_output / jnp.transpose(denominator, (2, 0, 1))[..., None]
    return attended.astype(jnp.bfloat16).reshape(length, -1)


def line_gather(piece, plane, planes):
    up = [(i, i + PLANE) for i in range(PLANE * (planes - 1))]
    down = [(i + PLANE, i) for i in range(PLANE * (planes - 1))]
    from_below, from_above = [piece], [piece]
    for _ in range(planes - 1):
        from_below.append(lax.ppermute(from_below[-1], "seq", up))
        from_above.append(lax.ppermute(from_above[-1], "seq", down))
    return [piece] + [
        jnp.where(plane + k < planes, from_above[k], from_below[planes - k])
        for k in range(1, planes)
    ]


def cyclic(x, begin, axis):
    return lax.dynamic_slice_in_dim(
        jnp.concatenate([x, x], axis=axis), begin, x.shape[axis], axis
    )


def attend_positions(queries, keys, vals, query_pos, key_pos, window):
    scores = jnp.einsum("bqhd,bkd->bhqk", queries, keys, preferred_element_type=jnp.float32)
    gap = query_pos[:, :, None] - key_pos[:, None, :]
    allowed = (gap >= 0) & (gap < window) & (key_pos[:, None, :] >= 0)
    weights = jnp.where(allowed[:, None], jnp.exp(scores), 0.0)
    denominator = jnp.sum(weights, axis=-1)
    mixed = jnp.einsum(
        "bhqk,bkd->bqhd", weights.astype(jnp.bfloat16), vals, preferred_element_type=jnp.float32
    )
    return (mixed / jnp.transpose(denominator, (0, 2, 1))[..., None]).astype(jnp.bfloat16)


def scatter_add(part, bits_first):
    def along_x(v):
        return v[0] + swap_seq(v[1].astype(jnp.bfloat16), 2).astype(jnp.float32)

    def along_y(v):
        return v[0] + swap_tp(v[1].astype(jnp.bfloat16)).astype(jnp.float32)

    if bits_first == "x":
        return along_y(along_x(part))
    return along_x(along_y(jnp.swapaxes(part, 0, 1)))


def local_plane(tokens, pre_gain, post_gain, w_query, key_matrix, value_matrix, w_out):
    seq = lax.axis_index("seq")
    n_seq = lax.axis_size("seq")
    planes = n_seq // PLANE
    plane = seq // PLANE
    tp = lax.axis_index("tp")
    own_rows, width = tokens.shape
    block = own_rows * lax.axis_size("tp")
    groups = [list(range(PLANE * i, PLANE * (i + 1))) for i in range(planes)]

    def trade(w, split_axis, concat_axis):
        return lax.all_to_all(
            w, "seq", split_axis=split_axis, concat_axis=concat_axis, tiled=True,
            axis_index_groups=groups,
        )

    depth = key_matrix.shape[0]
    kv = jnp.concatenate(
        [key_matrix.reshape(depth, PLANE, -1), value_matrix.reshape(depth, PLANE, -1)], axis=2
    ).reshape(depth, -1)
    w_kv = jnp.concatenate(line_gather(trade(kv, 1, 0), plane, planes), axis=0)
    w_q = jnp.concatenate(line_gather(trade(w_query, 1, 0), plane, planes), axis=0)
    out_piece = trade(w_out, 0, 1)
    span = out_piece.shape[1]
    cut = -(-span // 256) * 128
    w_o = [line_gather(out_piece[:, :cut], plane, planes), line_gather(out_piece[:, cut:], plane, planes)]

    normed = root_norm(tokens, pre_gain).astype(jnp.bfloat16)
    own = cyclic(normed, plane * span, 1)
    over_y = swap_tp(own)
    over_x = swap_seq(own, 2)
    half = own_rows // 2
    far = jnp.concatenate([swap_seq(over_y[:half], 2), swap_tp(over_x[half:])], axis=0)
    near_rows = jnp.concatenate([own, over_y, over_x, far], axis=0)
    far_rows = swap_seq(near_rows, 1)

    flips = [(dc + 2 * dx, dy) for dc in (0, 1) for dx in (0, 1) for dy in (0, 1)]
    begins = [(seq ^ s) * block + (tp ^ t) * own_rows for s, t in flips]
    positions = jnp.concatenate([b + jnp.arange(own_rows) for b in begins])
    float_pos = positions.astype(jnp.float32)

    raw_kv = jnp.concatenate(
        [jnp.dot(r, w_kv, preferred_element_type=jnp.float32) for r in (near_rows, far_rows)], axis=0
    )
    kv_width = raw_kv.shape[1] // 2
    keys = rotate_halves(raw_kv[:, :kv_width], float_pos).astype(jnp.bfloat16)
    kv_rows = jnp.concatenate([keys, raw_kv[:, kv_width:].astype(jnp.bfloat16)], axis=1)
    plane_rows = PLANE * block
    ordered = jnp.zeros((plane_rows, 2 * kv_width), jnp.bfloat16)
    for i, b in enumerate(begins):
        ordered = lax.dynamic_update_slice_in_dim(
            ordered, kv_rows[i * own_rows : (i + 1) * own_rows], b - plane * plane_rows, 0
        )
    prior = from_behind(ordered[plane_rows - block :], "seq", PLANE)
    window = jnp.concatenate([prior, ordered], axis=0)

    raw_q = jnp.concatenate(
        [jnp.dot(r, w_q, preferred_element_type=jnp.float32) for r in (near_rows, far_rows)], axis=0
    )
    queries = (rotate_halves(raw_q, float_pos) * HEAD_SIZE ** (-0.5)).astype(jnp.bfloat16)
    firsts = [seq ^ s for s in range(PLANE)]
    firsts = [firsts[0], firsts[2], firsts[1], firsts[3]]
    seen = jnp.stack(
        [
            lax.dynamic_slice_in_dim(window, (f - plane * PLANE) * block, 2 * block, 0)
            for f in firsts
        ]
    )
    key_pos = jnp.stack([(f - 1) * block + jnp.arange(2 * block) for f in firsts])
    attended = attend_positions(
        queries.reshape(PLANE, block, -1, HEAD_SIZE),
        seen[..., :kv_width],
        seen[..., kv_width:],
        positions.reshape(PLANE, block),
        key_pos,
        block,
    ).reshape(plane_rows, -1)

    sums = []
    for pieces in w_o:
        weights = jnp.concatenate(pieces, axis=1)
        theirs = jnp.dot(attended[plane_rows // 2 :], weights, preferred_element_type=jnp.float32)
        theirs = swap_seq(theirs.astype(jnp.bfloat16), 1)
        part = jnp.dot(attended[: plane_rows // 2], weights, preferred_element_type=jnp.float32)
        part = (part + theirs.astype(jnp.float32)).reshape(2, 2, own_rows, -1)
        middle = part.shape[3] // 2
        total = jnp.concatenate(
            [scatter_add(part[..., :middle], "x"), scatter_add(part[..., middle:], "y")], axis=1
        )
        sums.append(total.reshape(own_rows, planes, -1))
    projected = jnp.concatenate(sums, axis=2).reshape(own_rows, width)
    projected = cyclic(projected, (planes - plane) % planes * span, 1)
    mixed = root_norm(projected, post_gain)
    return (tokens.astype(jnp.float32) + mixed).astype(jnp.bfloat16)


def local(tokens, pre_gain, post_gain, w_query, key_matrix, value_matrix, w_out):
    block = tokens.shape[0] * lax.axis_size("tp")
    normalized_input = root_norm(tokens, pre_gain).astype(jnp.bfloat16)
    gathered = lax.all_gather(normalized_input, "tp", axis=0, tiled=True)
    pieces = (
        lax.all_gather(w_query, "seq", axis=0, tiled=True),
        lax.all_gather(key_matrix, "seq", axis=0, tiled=True),
        lax.all_gather(value_matrix, "seq", axis=0, tiled=True),
    )
    raw_q, raw_k, raw_v = tuple(
        (jnp.dot(gathered, piece, preferred_element_type=jnp.float32) for piece in pieces)
    )
    offset_pos = lax.axis_index("seq") * block
    token_positions = (offset_pos + jnp.arange(block)).astype(jnp.float32)
    query_rows = (rotate_halves(raw_q, token_positions) * HEAD_SIZE ** (-0.5)).astype(jnp.bfloat16)
    keys_now = rotate_halves(raw_k, token_positions).astype(jnp.bfloat16)
    vals_now = raw_v.astype(jnp.bfloat16)
    keys_prior, vals_prior = from_behind((keys_now, vals_now), "seq", 1)
    attended = attend(query_rows, keys_now, vals_now, keys_prior, vals_prior, offset_pos)
    partial_value = jnp.dot(
        attended,
        lax.all_gather(w_out, "seq", axis=1, tiled=True),
        preferred_element_type=jnp.float32,
    )
    own_rows = lax.psum_scatter(
        partial_value.astype(jnp.bfloat16), "tp", scatter_dimension=0, tiled=True
    ).astype(jnp.float32)
    mixed = root_norm(own_rows, post_gain)
    return (tokens.astype(jnp.float32) + mixed).astype(jnp.bfloat16)


def solution(mesh):
    def body(*args):
        kv_heads = args[4].shape[1] // HEAD_SIZE
        by_plane = kv_heads % PLANE == 0 and mesh.shape["seq"] % PLANE == 0 and mesh.shape["tp"] == 2
        return (local_plane if by_plane else local)(*args)

    return jax.shard_map(
        body,
        mesh=mesh,
        in_specs=(
            P(("seq", "tp"), None),
            P(),
            P(),
            P("seq", "tp"),
            P("seq", "tp"),
            P("seq", "tp"),
            P("tp", "seq"),
        ),
        out_specs=P(("seq", "tp"), None),
        check_vma=False,
    )
```

```python
import jax
import jax.numpy as jnp
from jax import lax
from jax.sharding import PartitionSpec as P

HEAD_SIZE = 256
PLANE = 4


def from_behind(x, axis, by):
    length = lax.axis_size(axis)
    pairs = [(i, i + by) for i in range(length) if 0 <= i + by < length]
    return lax.ppermute(x, axis, pairs)


def swap_seq(x, bits):
    return lax.ppermute(x, "seq", [(i, i ^ bits) for i in range(lax.axis_size("seq"))])


def swap_tp(x):
    return lax.ppermute(x, "tp", [(0, 1), (1, 0)])


def root_norm(values, gain):
    values = values.astype(jnp.float32)
    return values * lax.rsqrt(jnp.mean(values * values, axis=-1, keepdims=True) + 1e-06) * gain


def rotate_halves(values, token_positions):
    row_count = values.shape[0]
    shaped = values.reshape(row_count, -1, HEAD_SIZE)
    half_dim = HEAD_SIZE // 2
    freq = 10000.0 ** (-(jnp.arange(half_dim).astype(jnp.float32) * 2.0 / HEAD_SIZE))
    angle = token_positions[:, None] * freq[None, :]
    cosine = jnp.cos(angle)[:, None, :]
    sine_part = jnp.sin(angle)[:, None, :]
    first = shaped[..., :half_dim]
    second = shaped[..., half_dim:]
    turned = jnp.concatenate(
        [first * cosine - second * sine_part, second * cosine + first * sine_part], axis=-1
    )
    return turned.reshape(row_count, -1)


def attend(query_rows, keys_now, vals_now, keys_prior, vals_prior, offset_pos):
    length = query_rows.shape[0]
    kv_heads = keys_now.shape[1] // HEAD_SIZE
    repeat_heads = query_rows.shape[1] // (HEAD_SIZE * kv_heads)
    query_grouped = query_rows.reshape(length, kv_heads, repeat_heads, HEAD_SIZE)
    key_current = jnp.concatenate([keys_prior, keys_now], axis=0).reshape(
        2 * length, kv_heads, HEAD_SIZE
    )
    value_current = jnp.concatenate([vals_prior, vals_now], axis=0).reshape(
        2 * length, kv_heads, HEAD_SIZE
    )
    attention_scores = jnp.einsum(
        "cwap,bwp->wacb", query_grouped, key_current, preferred_element_type=jnp.float32
    )
    query_idx = jnp.arange(length)[:, None]
    key_idx = jnp.arange(2 * length)[None, :]
    key_pos = offset_pos - length + key_idx
    allowed = (key_idx > query_idx) & (key_idx <= query_idx + length) & (key_pos >= 0)
    weights = jnp.where(allowed, jnp.exp(attention_scores), 0.0)
    denominator = jnp.sum(weights, axis=-1)
    weight_narrow = weights.astype(jnp.bfloat16)
    reduced_output = jnp.einsum(
        "bpqu,ubm->qbpm", weight_narrow, value_current, preferred_element_type=jnp.float32
    )
    attended = reduced_output / jnp.transpose(denominator, (2, 0, 1))[..., None]
    return attended.astype(jnp.bfloat16).reshape(length, -1)


def hop(line):
    below, above = line
    devices = lax.axis_size("seq") - PLANE
    up = [(i, i + PLANE) for i in range(devices)]
    down = [(i + PLANE, i) for i in range(devices)]
    return (
        below + [lax.ppermute(below[-1], "seq", up)],
        above + [lax.ppermute(above[-1], "seq", down)],
    )


def hold(line, *others):
    below, above = line
    newest, *others = lax.optimization_barrier(((below[-1], above[-1]), *others))
    return (below[:-1] + [newest[0]], above[:-1] + [newest[1]]), *others


def line_pieces(line, plane):
    below, above = line
    planes = len(below)
    return [below[0]] + [
        jnp.where(plane + k < planes, above[k], below[planes - k]) for k in range(1, planes)
    ]


def cyclic(x, begin, axis):
    return lax.dynamic_slice_in_dim(
        jnp.concatenate([x, x], axis=axis), begin, x.shape[axis], axis
    )


def attend_positions(queries, keys, vals, query_pos, key_pos, window):
    scores = jnp.einsum("bqhd,bkd->bhqk", queries, keys, preferred_element_type=jnp.float32)
    gap = query_pos[:, :, None] - key_pos[:, None, :]
    allowed = (gap >= 0) & (gap < window) & (key_pos[:, None, :] >= 0)
    weights = jnp.where(allowed[:, None], jnp.exp(scores), 0.0)
    denominator = jnp.sum(weights, axis=-1)
    mixed = jnp.einsum(
        "bhqk,bkd->bqhd", weights.astype(jnp.bfloat16), vals, preferred_element_type=jnp.float32
    )
    return (mixed / jnp.transpose(denominator, (0, 2, 1))[..., None]).astype(jnp.bfloat16)


def scatter_add(part, bits_first):
    def along_x(v):
        return v[0] + swap_seq(v[1].astype(jnp.bfloat16), 2).astype(jnp.float32)

    def along_y(v):
        return v[0] + swap_tp(v[1].astype(jnp.bfloat16)).astype(jnp.float32)

    if bits_first == "x":
        return along_y(along_x(part))
    return along_x(along_y(jnp.swapaxes(part, 0, 1)))


def local_plane(tokens, pre_gain, post_gain, w_query, key_matrix, value_matrix, w_out):
    seq = lax.axis_index("seq")
    n_seq = lax.axis_size("seq")
    planes = n_seq // PLANE
    plane = seq // PLANE
    tp = lax.axis_index("tp")
    own_rows, width = tokens.shape
    block = own_rows * lax.axis_size("tp")
    groups = [list(range(PLANE * i, PLANE * (i + 1))) for i in range(planes)]

    def trade(w, split_axis, concat_axis):
        return lax.all_to_all(
            w, "seq", split_axis=split_axis, concat_axis=concat_axis, tiled=True,
            axis_index_groups=groups,
        )

    depth = key_matrix.shape[0]
    kv = jnp.concatenate(
        [key_matrix.reshape(depth, PLANE, -1), value_matrix.reshape(depth, PLANE, -1)], axis=2
    ).reshape(depth, -1)
    inner_hops = planes - 3

    kv_piece = trade(kv, 1, 0)
    w_query, kv_piece = lax.optimization_barrier((w_query, kv_piece))
    q_piece = trade(w_query, 1, 0)
    w_out, q_piece = lax.optimization_barrier((w_out, q_piece))
    out_piece = trade(w_out, 0, 1)
    span = out_piece.shape[1]
    cut = -(-span // 256) * 128

    normed = root_norm(tokens, pre_gain).astype(jnp.bfloat16)
    own = cyclic(normed, plane * span, 1)
    over_y = swap_tp(own)
    over_x = swap_seq(own, 2)
    kv_line = hop(([kv_piece], [kv_piece]))
    kv_line, over_y, over_x = hold(kv_line, over_y, over_x)
    half = own_rows // 2
    far = jnp.concatenate([swap_seq(over_y[:half], 2), swap_tp(over_x[half:])], axis=0)
    for _ in range(inner_hops):
        kv_line = hop(kv_line)
    kv_line, far = hold(kv_line, far)
    near_rows = jnp.concatenate([own, over_y, over_x, far], axis=0)
    far_rows = swap_seq(near_rows, 1)

    kv_line, q_newest = hold(kv_line, (q_piece, q_piece))
    q_line = ([q_newest[0]], [q_newest[1]])
    kv_line = hop(kv_line)
    q_line = hop(q_line)
    w_kv = jnp.concatenate(line_pieces(kv_line, plane), axis=0)

    flips = [(dc + 2 * dx, dy) for dc in (0, 1) for dx in (0, 1) for dy in (0, 1)]
    begins = [(seq ^ s) * block + (tp ^ t) * own_rows for s, t in flips]
    positions = jnp.concatenate([b + jnp.arange(own_rows) for b in begins])
    float_pos = positions.astype(jnp.float32)

    raw_kv = [jnp.dot(r, w_kv, preferred_element_type=jnp.float32) for r in (near_rows, far_rows)]
    q_line, raw_kv = hold(q_line, raw_kv)
    for _ in range(inner_hops):
        q_line = hop(q_line)
    raw_kv = jnp.concatenate(raw_kv, axis=0)
    kv_width = raw_kv.shape[1] // 2
    keys = rotate_halves(raw_kv[:, :kv_width], float_pos).astype(jnp.bfloat16)
    kv_rows = jnp.concatenate([keys, raw_kv[:, kv_width:].astype(jnp.bfloat16)], axis=1)
    plane_rows = PLANE * block
    ordered = jnp.zeros((plane_rows, 2 * kv_width), jnp.bfloat16)
    for i, b in enumerate(begins):
        ordered = lax.dynamic_update_slice_in_dim(
            ordered, kv_rows[i * own_rows : (i + 1) * own_rows], b - plane * plane_rows, 0
        )
    piece = out_piece[:, :cut]
    q_line, ordered, piece = hold(q_line, ordered, piece)
    prior = from_behind(ordered[plane_rows - block :], "seq", PLANE)
    window = jnp.concatenate([prior, ordered], axis=0)

    q_line = hop(q_line)
    first_line = hop(([piece], [piece]))
    w_q = jnp.concatenate(line_pieces(q_line, plane), axis=0)
    raw_q = [jnp.dot(r, w_q, preferred_element_type=jnp.float32) for r in (near_rows, far_rows)]
    first_line, raw_q = hold(first_line, raw_q)
    for _ in range(inner_hops):
        first_line = hop(first_line)
    piece = out_piece[:, cut:]
    first_line, piece = hold(first_line, piece)
    first_line = hop(first_line)
    second_line = hop(([piece], [piece]))
    w_first = jnp.concatenate(line_pieces(first_line, plane), axis=1)
    raw_q = jnp.concatenate(raw_q, axis=0)
    queries = (rotate_halves(raw_q, float_pos) * HEAD_SIZE ** (-0.5)).astype(jnp.bfloat16)
    firsts = [seq ^ s for s in range(PLANE)]
    firsts = [firsts[0], firsts[2], firsts[1], firsts[3]]
    seen = jnp.stack(
        [
            lax.dynamic_slice_in_dim(window, (f - plane * PLANE) * block, 2 * block, 0)
            for f in firsts
        ]
    )
    key_pos = jnp.stack([(f - 1) * block + jnp.arange(2 * block) for f in firsts])
    attended = attend_positions(
        queries.reshape(PLANE, block, -1, HEAD_SIZE),
        seen[..., :kv_width],
        seen[..., kv_width:],
        positions.reshape(PLANE, block),
        key_pos,
        block,
    ).reshape(plane_rows, -1)

    def for_other_core(weights):
        product = jnp.dot(attended[plane_rows // 2 :], weights, preferred_element_type=jnp.float32)
        return product.astype(jnp.bfloat16)

    first = for_other_core(w_first)
    second_line, first = hold(second_line, first)
    first = swap_seq(first, 1)
    for _ in range(inner_hops):
        second_line = hop(second_line)
    second_line, first = hold(second_line, first)
    second_line = hop(second_line)
    w_second = jnp.concatenate(line_pieces(second_line, plane), axis=1)
    second = swap_seq(for_other_core(w_second), 1)
    sums = []
    for weights, theirs in ((w_first, first), (w_second, second)):
        part = jnp.dot(attended[: plane_rows // 2], weights, preferred_element_type=jnp.float32)
        part = (part + theirs.astype(jnp.float32)).reshape(2, 2, own_rows, -1)
        middle = part.shape[3] // 2
        total = jnp.concatenate(
            [scatter_add(part[..., :middle], "x"), scatter_add(part[..., middle:], "y")], axis=1
        )
        sums.append(total.reshape(own_rows, planes, -1))
    projected = jnp.concatenate(sums, axis=2).reshape(own_rows, width)
    projected = cyclic(projected, (planes - plane) % planes * span, 1)
    mixed = root_norm(projected, post_gain)
    return (tokens.astype(jnp.float32) + mixed).astype(jnp.bfloat16)


def local(tokens, pre_gain, post_gain, w_query, key_matrix, value_matrix, w_out):
    block = tokens.shape[0] * lax.axis_size("tp")
    normalized_input = root_norm(tokens, pre_gain).astype(jnp.bfloat16)
    gathered = lax.all_gather(normalized_input, "tp", axis=0, tiled=True)
    pieces = (
        lax.all_gather(w_query, "seq", axis=0, tiled=True),
        lax.all_gather(key_matrix, "seq", axis=0, tiled=True),
        lax.all_gather(value_matrix, "seq", axis=0, tiled=True),
    )
    raw_q, raw_k, raw_v = tuple(
        (jnp.dot(gathered, piece, preferred_element_type=jnp.float32) for piece in pieces)
    )
    offset_pos = lax.axis_index("seq") * block
    token_positions = (offset_pos + jnp.arange(block)).astype(jnp.float32)
    query_rows = (rotate_halves(raw_q, token_positions) * HEAD_SIZE ** (-0.5)).astype(jnp.bfloat16)
    keys_now = rotate_halves(raw_k, token_positions).astype(jnp.bfloat16)
    vals_now = raw_v.astype(jnp.bfloat16)
    keys_prior, vals_prior = from_behind((keys_now, vals_now), "seq", 1)
    attended = attend(query_rows, keys_now, vals_now, keys_prior, vals_prior, offset_pos)
    partial_value = jnp.dot(
        attended,
        lax.all_gather(w_out, "seq", axis=1, tiled=True),
        preferred_element_type=jnp.float32,
    )
    own_rows = lax.psum_scatter(
        partial_value.astype(jnp.bfloat16), "tp", scatter_dimension=0, tiled=True
    ).astype(jnp.float32)
    mixed = root_norm(own_rows, post_gain)
    return (tokens.astype(jnp.float32) + mixed).astype(jnp.bfloat16)


def solution(mesh):
    def body(*args):
        kv_heads = args[4].shape[1] // HEAD_SIZE
        planes, rest = divmod(mesh.shape["seq"], PLANE)
        by_plane = kv_heads % PLANE == 0 and rest == 0 and planes >= 3 and mesh.shape["tp"] == 2
        return (local_plane if by_plane else local)(*args)

    return jax.shard_map(
        body,
        mesh=mesh,
        in_specs=(
            P(("seq", "tp"), None),
            P(),
            P(),
            P("seq", "tp"),
            P("seq", "tp"),
            P("seq", "tp"),
            P("tp", "seq"),
        ),
        out_specs=P(("seq", "tp"), None),
        check_vma=False,
    )
```

```python
import jax
import jax.numpy as jnp
from jax import lax
from jax.sharding import PartitionSpec as P

HEAD_SIZE = 256
BLOCK_TOKENS = 512


def from_behind(x, axis, by):
    length = lax.axis_size(axis)
    pairs = [(i, i + by) for i in range(length) if 0 <= i + by < length]
    return lax.ppermute(x, axis, pairs)


def root_norm(values, gain):
    values = values.astype(jnp.float32)
    return values * lax.rsqrt(jnp.mean(values * values, axis=-1, keepdims=True) + 1e-06) * gain


def rotate_halves(values, token_positions):
    row_count = values.shape[0]
    shaped = values.reshape(row_count, -1, HEAD_SIZE)
    half_dim = HEAD_SIZE // 2
    freq = 10000.0 ** (-(jnp.arange(half_dim).astype(jnp.float32) * 2.0 / HEAD_SIZE))
    angle = token_positions[:, None] * freq[None, :]
    cosine = jnp.cos(angle)[:, None, :]
    sine_part = jnp.sin(angle)[:, None, :]
    first = shaped[..., :half_dim]
    second = shaped[..., half_dim:]
    turned = jnp.concatenate(
        [first * cosine - second * sine_part, second * cosine + first * sine_part], axis=-1
    )
    return turned.reshape(row_count, -1)


def attend(query_rows, keys_now, vals_now, keys_prior, vals_prior, offset_pos):
    length = query_rows.shape[0]
    kv_heads = keys_now.shape[1] // HEAD_SIZE
    repeat_heads = query_rows.shape[1] // (HEAD_SIZE * kv_heads)
    query_grouped = query_rows.reshape(length, kv_heads, repeat_heads, HEAD_SIZE)
    key_current = jnp.concatenate([keys_prior, keys_now], axis=0).reshape(
        2 * length, kv_heads, HEAD_SIZE
    )
    value_current = jnp.concatenate([vals_prior, vals_now], axis=0).reshape(
        2 * length, kv_heads, HEAD_SIZE
    )
    attention_scores = jnp.einsum(
        "cwap,bwp->wacb", query_grouped, key_current, preferred_element_type=jnp.float32
    )
    query_idx = jnp.arange(length)[:, None]
    key_idx = jnp.arange(2 * length)[None, :]
    key_pos = offset_pos - length + key_idx
    allowed = (key_idx > query_idx) & (key_idx <= query_idx + length) & (key_pos >= 0)
    weights = jnp.where(allowed, jnp.exp(attention_scores), 0.0)
    denominator = jnp.sum(weights, axis=-1)
    weight_narrow = weights.astype(jnp.bfloat16)
    reduced_output = jnp.einsum(
        "bpqu,ubm->qbpm", weight_narrow, value_current, preferred_element_type=jnp.float32
    )
    attended = reduced_output / jnp.transpose(denominator, (2, 0, 1))[..., None]
    return attended.astype(jnp.bfloat16).reshape(length, -1)


def local(tokens, pre_gain, post_gain, w_query, key_matrix, value_matrix, w_out):
    normalized_input = root_norm(tokens, pre_gain).astype(jnp.bfloat16)
    tp = lax.axis_index("tp")
    two = lax.axis_size("tp") == 2
    if two:
        peer = lax.ppermute(normalized_input, "tp", [(0, 1), (1, 0)])
        gathered = jnp.where(
            tp == 0,
            jnp.concatenate([normalized_input, peer], axis=0),
            jnp.concatenate([peer, normalized_input], axis=0),
        )
    else:
        gathered = lax.all_gather(normalized_input, "tp", axis=0, tiled=True)
    pieces = (
        lax.all_gather(w_query, "seq", axis=0, tiled=True),
        lax.all_gather(key_matrix, "seq", axis=0, tiled=True),
        lax.all_gather(value_matrix, "seq", axis=0, tiled=True),
    )
    raw_q, raw_k, raw_v = tuple(
        (jnp.dot(gathered, piece, preferred_element_type=jnp.float32) for piece in pieces)
    )
    offset_pos = lax.axis_index("seq") * BLOCK_TOKENS
    token_positions = (offset_pos + jnp.arange(BLOCK_TOKENS)).astype(jnp.float32)
    query_rows = (rotate_halves(raw_q, token_positions) * HEAD_SIZE ** (-0.5)).astype(jnp.bfloat16)
    keys_now = rotate_halves(raw_k, token_positions).astype(jnp.bfloat16)
    vals_now = raw_v.astype(jnp.bfloat16)
    keys_prior, vals_prior = from_behind((keys_now, vals_now), "seq", 1)
    attended = attend(query_rows, keys_now, vals_now, keys_prior, vals_prior, offset_pos)
    partial_value = jnp.dot(
        attended,
        lax.all_gather(w_out, "seq", axis=1, tiled=True),
        preferred_element_type=jnp.float32,
    )
    if two:
        count = tokens.shape[0]
        kept = lax.dynamic_slice_in_dim(partial_value, tp * count, count, 0)
        sent = lax.dynamic_slice_in_dim(partial_value, (1 - tp) * count, count, 0)
        came = lax.ppermute(sent.astype(jnp.bfloat16), "tp", [(0, 1), (1, 0)])
        own_rows = kept.astype(jnp.bfloat16).astype(jnp.float32) + came.astype(jnp.float32)
    else:
        own_rows = lax.psum_scatter(
            partial_value.astype(jnp.bfloat16), "tp", scatter_dimension=0, tiled=True
        ).astype(jnp.float32)
    mixed = root_norm(own_rows, post_gain)
    return (tokens.astype(jnp.float32) + mixed).astype(jnp.bfloat16)


def solution(mesh):
    return jax.shard_map(
        local,
        mesh=mesh,
        in_specs=(
            P(("seq", "tp"), None),
            P(),
            P(),
            P("seq", "tp"),
            P("seq", "tp"),
            P("seq", "tp"),
            P("tp", "seq"),
        ),
        out_specs=P(("seq", "tp"), None),
        check_vma=False,
    )
```
